128 devices in a mesh: dp: 128 (over z, y, x, core).
Axes of the slice: x: 4, y: 4, z: 4, core: 2. Of those that a mesh axis runs over, the one named last changes fastest.
Arguments:
- grads: float32 [128, 4194304], P('dp')
- master: float32 [4194304], P('dp'), may hold values from -0.75 to 0.75
- m_old: float32 [128, 65536], P('dp'), may hold values from -6 to 6
- v_old: float32 [128, 65536], P('dp'), may hold values from 0.25 to 4
- old_bounds: int32 [129], replicated, may hold values from 0 to 4194304, as said below
Outputs:
- master_new: float32 [4194304], P('dp')
- m_new: float32 [4194304], P('dp')
- v_new: float32 [4194304], P('dp')
- params_full: bfloat16 [4194304], replicated
The draws below stay inside these ranges and needn't reach their ends.
Inputs may be any that keep to these rules, and one draw needn't show every extreme that they name: old_bounds[0] = 0, the last entry is 4194304, entries never fall, and old_bounds[i] - i * 32768 lies between -16384 and 16384 for every i. Row k of m_old and v_old holds its span in its first old_bounds[k+1] - old_bounds[k] slots; later slots are unused. Some span has exactly 65536 entries in every draw.
All inputs are finite; a program needn't handle non-finite values.
Results may differ from the reference program's by a relative error of at most 0.0049.
Values may be sent and summed in bfloat16 or wider, within the bound.
A program may use at most 128 MiB of HBM per device.

```python
import math
import jax
import jax.numpy as jnp
from jax import lax

ND = 32768
FLAT = 4194304
CAP = 65536
N_DP = 128


def draw_grads(key, part):
    first = jax.random.fold_in(jax.random.fold_in(key, 21), 0)
    fourth = jax.random.fold_in(jax.random.fold_in(key, 21), 3)
    fifth = jax.random.fold_in(jax.random.fold_in(key, 21), 4)
    positions = jnp.arange(FLAT, dtype=jnp.float32)
    ramp = 1.0 + 2.0 * positions / FLAT
    block_level = jnp.exp(jax.random.uniform(fourth, (N_DP, 1), jnp.float32, -0.8, 0.8))
    level = (block_level * jnp.ones((1, ND), jnp.float32)).reshape(FLAT)
    overall = jnp.exp(jax.random.uniform(fifth, (), jnp.float32, -1.0, 1.0))
    values = jax.random.normal(first, (N_DP, FLAT), jnp.float32) * (ramp * level * overall)
    return values.astype(jnp.float32)


def draw_old_bounds(key, part):
    first, second = jax.random.split(jax.random.fold_in(key, 11))
    margin = ND // 2
    drift = jax.random.randint(first, (N_DP + 1,), -margin, margin + 1)
    chosen = jax.random.randint(second, (), 1, N_DP - 1)
    index_all = jnp.arange(N_DP + 1, dtype=jnp.int32)
    drift = jnp.where(index_all == chosen, -margin, drift)
    drift = jnp.where(index_all == chosen + 1, margin, drift)
    drift = jnp.where((index_all == 0) | (index_all == N_DP), 0, drift)
    return (index_all * ND + drift).astype(jnp.int32)


def block_scale(stream_key, extent, cuts, low, largest):
    loudness, own = 1.0, jax.random.fold_in(stream_key, 6)
    for position, shards_of in cuts:
        heights = jnp.exp(jax.random.uniform(jax.random.fold_in(own, position), (shards_of,), jnp.float32, low / len(cuts), largest / len(cuts)))
        loudness = loudness * jnp.repeat(heights, extent[position] // shards_of).reshape([-1 if axis == position else 1 for axis in range(len(extent))])
    return loudness


def centred(stream_key, dims, deviation, bound, shards=(), kind=jnp.bfloat16):
    drawn = jax.random.normal(stream_key, dims, jnp.float32) * deviation
    if len(shards) > 0:
        drawn = block_scale(stream_key, dims, shards, -0.22, 0.18) * drawn
    return jnp.clip(drawn, min=-bound, max=bound).astype(kind)


def setup_inputs(seed: int = 0) -> dict:
    key_list = jax.random.split(jax.random.key(seed), 6)
    return {
        "grads": draw_grads(jax.random.fold_in(key_list[5], 71), 0),
        "master": centred(key_list[1], (FLAT,), 0.05, 0.75, ((0, 128),), jnp.float32),
        "m_old": centred(key_list[2], (N_DP, CAP), 1.0, 6.0, ((0, 128),), jnp.float32),
        "v_old": jnp.clip(jnp.exp(math.log(4.0) - 2.7725887 * jax.random.uniform(key_list[3], (N_DP, CAP), jnp.float32) ** block_scale(key_list[3], (N_DP, CAP), ((0, 128),), -0.2, 0.2)), 0.25, 4.0),
        "old_bounds": draw_old_bounds(jax.random.fold_in(key_list[5], 71), 0),
    }


def reference(grads, master, m_old, v_old, old_bounds):
    gradient = lax.optimization_barrier(jnp.sum(grads, axis=0))
    positions = jnp.arange(FLAT, dtype=jnp.int32)
    owner = (jnp.searchsorted(old_bounds, positions, side='right') - 1).astype(jnp.int32)
    slot = (positions - old_bounds[owner]).astype(jnp.int32)
    m_prev = m_old[owner, slot]
    v_prev = v_old[owner, slot]
    total = jnp.sum(gradient * gradient)
    clip = jnp.minimum(1.0, jnp.sqrt(jnp.float32(FLAT)) / (jnp.sqrt(total) + 1e-06))
    clipped = clip * gradient
    m_new = 0.5 * m_prev + 0.5 * clipped
    v_new = 0.95 * v_prev + 0.05 * clipped * clipped
    direction = m_new / (1.0 - 0.5 ** 20) / (jnp.sqrt(v_new / (1.0 - 0.95 ** 20)) + 1e-08)
    master_new = master - 0.05 * (direction + 0.1 * master)
    return (master_new, m_new, v_new, master_new.astype(jnp.bfloat16))
```

```python
import jax
import jax.numpy as jnp
from jax import lax
from jax.experimental import pallas as pl
from jax.experimental.pallas import tpu as pltpu
from jax.sharding import Mesh
from jax.sharding import PartitionSpec as P

DP = ("dz", "dy", "dx", "dc")
F32, BF16 = jnp.float32, jnp.bfloat16
LANES = 128
ORDERS = ((2, 1, 0), (1, 0, 2), (0, 2, 1))
HALVES = ((48, 48), (48, 48), (32, 32))
SLOTS = (2, 1, 3, 0)
FAR, DIRECT, RELAY = 0, 1, 2


def plan(rows):
    spans, at = [], 0
    for pair in HALVES:
        colour = []
        for part in pair:
            size = part * rows // 256
            colour.append((at, size))
            at += size
        spans.append(colour)
    return spans


def kernel(spans, rows, refs):
    g, master, window, tail, head, bounds = refs["in"]
    master_out, m_out, v_out, params = refs["out"]
    s = refs["scratch"]
    coords = [lax.axis_index(name) for name in DP[:3]]
    core = lax.axis_index("dc")
    other = 1 - core
    me = ((coords[0] * 4 + coords[1]) * 4 + coords[2]) * 2 + core

    def moved(dim, steps):
        at = list(coords)
        at[dim] = (coords[dim] + steps + 4) % 4
        return (*at, core)

    def located(index):
        return (index // 32, (index // 8) % 4, (index // 2) % 4, index % 2)

    partner = (*coords, other)
    after, before = located((me + 1) % 128), located((me + 127) % 128)
    beside = located((me + 127 + 2 * core) % 128)

    def remote(src, dst, send, recv, device):
        return pltpu.make_async_remote_copy(
            src_ref=src, dst_ref=dst, send_sem=send, recv_sem=recv, device_id=device, device_id_type=pl.DeviceIdType.MESH
        )

    def source(k, slot, parity):
        first = ORDERS[k][0]
        at = [slice(None)] * 3
        at[first] = (coords[first] + slot) % 4
        low = spans[k][0][0]
        size = spans[k][0][1] + spans[k][1][1]
        return g.at[at[0], at[1], at[2], parity, pl.ds(low, size)]

    loads = {}
    for slot in SLOTS:
        for k in range(3):
            loads[k, slot, 1] = pltpu.make_async_copy(source(k, slot, other), s["theirs"][k].at[slot], s["load"].at[k, slot, 1])
            loads[k, slot, 0] = pltpu.make_async_copy(source(k, slot, core), s["ours"][k].at[slot], s["load"].at[k, slot, 0])
            loads[k, slot, 1].start()
            loads[k, slot, 0].start()
    small = [
        pltpu.make_async_copy(master, s["master"], s["small"].at[0]),
        pltpu.make_async_copy(window, s["window"], s["small"].at[1]),
    ]
    for copy in small:
        copy.start()

    barrier = pltpu.get_barrier_semaphore()
    peers = [moved(dim, step) for dim in range(3) for step in (1, 2, 3)] + [partner, beside]
    for peer in peers:
        pl.semaphore_signal(barrier, inc=1, device_id=peer, device_id_type=pl.DeviceIdType.MESH)
    pl.semaphore_wait(barrier, len(peers))

    pending = []

    def launch(copy):
        copy.start()
        pending.append(copy)
        return copy

    swaps = {}
    for slot in range(4):
        for k in range(3):
            swaps[k, slot] = remote(
                s["give"][k].at[slot], s["take"][k].at[slot], s["swap_out"].at[k, slot], s["swap_in"].at[k, slot], partner
            )

    def narrow(k, slot):
        loads[k, slot, 1].wait()

        def body(t, carry):
            s["give"][k][slot, t // 4, t % 4] = s["theirs"][k][slot, t // 4, t % 4].astype(BF16)
            return carry

        lax.fori_loop(0, 16, body, 0)
        launch(swaps[k, slot])

    def joined(k, slot, h, t):
        u, v = (t // 4, t % 4) if ORDERS[k][1] < ORDERS[k][2] else (t % 4, t // 4)
        low = spans[k][h][0] - spans[k][0][0]
        at = pl.ds(low, spans[k][h][1])
        return s["ours"][k][slot, u, v, at] + s["take"][k][slot, u, v, at].astype(F32)

    def arrive(k, slot):
        loads[k, slot, 0].wait()
        swaps[k, slot].wait_recv()

    streams = [(k, h) for k in range(3) for h in range(2)]
    sign = {0: 1, 1: -1}

    rs = {}
    for q, (k, h) in enumerate(streams):
        for phase in range(3):
            dim = ORDERS[k][phase]
            for kind, step in ((FAR, sign[h]), (DIRECT, -sign[h]), (RELAY, sign[h])):
                rs[q, phase, kind] = remote(
                    s["out"][q][phase].at[kind],
                    s["in"][q][phase].at[kind],
                    s["rs_out"].at[q, phase, kind],
                    s["rs_in"].at[q, phase, kind],
                    moved(dim, step),
                )

    def loop(count, body):
        def step(t, carry):
            body(t)
            return carry

        lax.fori_loop(0, count, step, 0)

    for k in range(3):
        narrow(k, 2)
    for k in range(3):
        narrow(k, 3)
        arrive(k, 2)
        for h in range(2):
            q = 2 * k + h

            def body(t, k=k, h=h, q=q):
                s["out"][q][0][FAR, t] = joined(k, 2, h, t).astype(BF16)

            loop(16, body)
            launch(rs[q, 0, FAR])
    for k in range(3):
        narrow(k, 1)
    for h, slot in ((0, 3), (1, 1)):
        for k in range(3):
            q = 2 * k + h
            arrive(k, slot)

            def body(t, k=k, h=h, q=q, slot=slot):
                s["out"][q][0][DIRECT, t] = joined(k, slot, h, t).astype(BF16)

            loop(16, body)
            launch(rs[q, 0, DIRECT])
    for k in range(3):
        narrow(k, 0)
    moments_out = [
        launch(remote(tail, s["from_before"], s["mom_out"].at[0], s["mom_in"].at[0], after)),
        launch(remote(head, s["from_after"], s["mom_out"].at[1], s["mom_in"].at[1], before)),
    ]
    for q, (k, h) in enumerate(streams):
        rs[q, 0, FAR].wait_recv()

        def body(t, k=k, h=h, q=q):
            value = joined(k, sign[h] % 4, h, t) + s["in"][q][0][FAR, t].astype(F32)
            s["out"][q][0][RELAY, t] = value.astype(BF16)

        loop(16, body)
        launch(rs[q, 0, RELAY])

    for copy in small:
        copy.wait()
    for copy in moments_out:
        copy.wait_recv()
    start = me * (rows * LANES)
    low, high = bounds[me] - start, bounds[me + 1] - start
    place = lax.broadcasted_iota(jnp.int32, (rows // 2, LANES), 0) * LANES + lax.broadcasted_iota(
        jnp.int32, (rows // 2, LANES), 1
    )
    for i in range(2):
        top, bottom = pl.ds(0, rows // 2), pl.ds(rows // 2, rows // 2)
        s["window"][i, top] = jnp.where(place < low, s["from_before"][i].astype(F32), s["window"][i, top])
        s["window"][i, bottom] = jnp.where(
            place + (rows // 2) * LANES >= high, s["from_after"][i].astype(F32), s["window"][i, bottom]
        )

    for k in range(3):
        arrive(k, 0)
    for q, (k, h) in enumerate(streams):
        rs[q, 0, DIRECT].wait_recv()
        rs[q, 0, RELAY].wait_recv()

        def body(t, k=k, h=h, q=q):
            got = s["in"][q][0]
            s["sum"][q][0][t] = joined(k, 0, h, t) + got[DIRECT, t].astype(F32) + got[RELAY, t].astype(F32)

        loop(16, body)
        if True:
            second(s, rs, launch, loop, coords, q, k, h, sign, 1, 4)
    for q, (k, h) in enumerate(streams):
        relay(s, rs, launch, loop, coords, q, k, h, sign, 1, 4)
    for q, (k, h) in enumerate(streams):
        finish(s, rs, loop, coords, q, k, 1, 4)
        second(s, rs, launch, loop, coords, q, k, h, sign, 2, 1)
    for q, (k, h) in enumerate(streams):
        relay(s, rs, launch, loop, coords, q, k, h, sign, 2, 1)
    total = jnp.zeros((8, LANES), F32)
    for q, (k, h) in enumerate(streams):
        finish(s, rs, loop, coords, q, k, 2, 1)
        value = s["sum"][q][2][0]
        square = value * value
        for i in range(spans[k][h][1] // 8):
            total += square[8 * i : 8 * i + 8]

    s["norm"][0] = total
    copy = launch(remote(s["norm"].at[0], s["norm_in"].at[0], s["norm_out"].at[0], s["norm_got"].at[0], partner))
    copy.wait_recv()
    s["norm"][1] = s["norm"][0] + s["norm_in"][0]
    for dim in range(3):
        copies = [
            launch(
                remote(
                    s["norm"].at[1 + dim],
                    s["norm_in"].at[3 * dim + step],
                    s["norm_out"].at[3 * dim + step],
                    s["norm_got"].at[3 * dim + step],
                    moved(dim, step),
                )
            )
            for step in (1, 2, 3)
        ]
        value = s["norm"][1 + dim]
        for step, copy in zip((1, 2, 3), copies):
            copy.wait_recv()
            value += s["norm_in"][3 * dim + step]
        s["norm"][2 + dim] = value
    norm = jnp.sum(s["norm"][4], axis=(0, 1), keepdims=True)
    clip = jnp.minimum(1.0, jnp.sqrt(F32(128 * rows * LANES)) / (jnp.sqrt(norm) + 1e-06))

    for q, (k, h) in enumerate(streams):
        at = pl.ds(*spans[k][h])
        clipped = clip * s["sum"][q][2][0]
        m_new = 0.5 * s["window"][0, at] + 0.5 * clipped
        v_new = 0.95 * s["window"][1, at] + 0.05 * clipped * clipped
        direction = m_new / (1.0 - 0.5**20) / (jnp.sqrt(v_new / (1.0 - 0.95**20)) + 1e-08)
        weights = s["master"][at]
        weights = weights - 0.05 * (direction + 0.1 * weights)
        master_out[at] = weights
        m_out[at] = m_new
        v_out[at] = v_new
        params[coords[0], coords[1], coords[2], core, at] = weights.astype(BF16)

    def piece(k, fixed, low, size):
        at = [fixed.get(dim, slice(None)) for dim in range(3)]
        return params.at[at[0], at[1], at[2], core, pl.ds(low, size)]

    def fixed_at(k, stage, step):
        order = ORDERS[k][::-1]
        fixed = {dim: coords[dim] for dim in order[stage:]}
        fixed[order[stage]] = (coords[order[stage]] + step + 4) % 4
        return fixed

    def sent(ref, sem, device):
        return remote(ref, ref, s["ag_out"].at[sem], s["ag_in"].at[sem], device)

    def sem_of(k, stage, i):
        return (k * 3 + stage) * 4 + i

    shared = []

    def share(k, stage, step):
        low = spans[k][0][0]
        size = spans[k][0][1] + spans[k][1][1]
        i = len(shared)
        ref = piece(k, fixed_at(k, stage, step), low, size)
        shared.append(launch(remote(ref, ref, s["share_out"].at[i], s["share_in"].at[i], partner)))

    for k in range(3):
        share(k, 0, 0)
    for stage in range(3):
        hops = {}
        for k in range(3):
            dim = ORDERS[k][::-1][stage]
            low, size = spans[k][0][0], spans[k][0][1] + spans[k][1][1]
            ref = piece(k, fixed_at(k, stage, 0), low, size)
            for i, step in ((0, 1), (1, -1)):
                hops[k, i] = launch(sent(ref, sem_of(k, stage, i), moved(dim, step)))
        for k in range(3):
            dim = ORDERS[k][::-1][stage]
            for i, step in ((0, 1), (1, -1)):
                hops[k, i].wait_recv()
                ref = piece(k, fixed_at(k, stage, -step), *spans[k][i])
                hops[k, 2 + i] = launch(sent(ref, sem_of(k, stage, 2 + i), moved(dim, step)))
                share(k, stage, -step)
        for k in range(3):
            hops[k, 2].wait_recv()
            hops[k, 3].wait_recv()
            share(k, stage, 2)
    for copy in shared:
        copy.wait_recv()
    for copy in pending:
        copy.wait_send()


def second(s, rs, launch, loop, coords, q, k, h, sign, phase, count):
    place = coords[ORDERS[k][phase]]
    for kind, step in ((FAR, 2), (DIRECT, -sign[h])):
        at = ((place + step + 4) % 4) * count

        def body(t, kind=kind, at=at):
            s["out"][q][phase][kind, t] = s["sum"][q][phase - 1][at + t].astype(BF16)

        loop(count, body)
        launch(rs[q, phase, kind])


def relay(s, rs, launch, loop, coords, q, k, h, sign, phase, count):
    place = coords[ORDERS[k][phase]]
    rs[q, phase, FAR].wait_recv()
    at = ((place + sign[h] + 4) % 4) * count

    def body(t):
        value = s["sum"][q][phase - 1][at + t] + s["in"][q][phase][FAR, t].astype(F32)
        s["out"][q][phase][RELAY, t] = value.astype(BF16)

    loop(count, body)
    launch(rs[q, phase, RELAY])


def finish(s, rs, loop, coords, q, k, phase, count):
    place = coords[ORDERS[k][phase]]
    rs[q, phase, DIRECT].wait_recv()
    rs[q, phase, RELAY].wait_recv()
    at = place * count

    def body(t):
        got = s["in"][q][phase]
        s["sum"][q][phase][t] = s["sum"][q][phase - 1][at + t] + got[DIRECT, t].astype(F32) + got[RELAY, t].astype(F32)

    loop(count, body)


def step(g, master, window, tail, head, bounds):
    rows = master.shape[0]
    spans = plan(rows)
    sizes = [a[1] + b[1] for a, b in spans]
    dma = pltpu.SemaphoreType.DMA
    halves = [span for colour in spans for span in colour]
    scratch = {
        "theirs": [pltpu.VMEM((4, 4, 4, n, LANES), F32) for n in sizes],
        "ours": [pltpu.VMEM((4, 4, 4, n, LANES), F32) for n in sizes],
        "give": [pltpu.VMEM((4, 4, 4, n, LANES), BF16) for n in sizes],
        "take": [pltpu.VMEM((4, 4, 4, n, LANES), BF16) for n in sizes],
        "out": [[pltpu.VMEM((3, m, n, LANES), BF16) for m in (16, 4, 1)] for _, n in halves],
        "in": [[pltpu.VMEM((3, m, n, LANES), BF16) for m in (16, 4, 1)] for _, n in halves],
        "sum": [[pltpu.VMEM((m, n, LANES), F32) for m in (16, 4, 1)] for _, n in halves],
        "master": pltpu.VMEM((rows, LANES), F32),
        "window": pltpu.VMEM((2, rows, LANES), F32),
        "from_before": pltpu.VMEM((2, rows // 2, LANES), BF16),
        "from_after": pltpu.VMEM((2, rows // 2, LANES), BF16),
        "norm": pltpu.VMEM((5, 8, LANES), F32),
        "norm_in": pltpu.VMEM((10, 8, LANES), F32),
        "load": dma((3, 4, 2)),
        "small": dma((2,)),
        "swap_out": dma((3, 4)),
        "swap_in": dma((3, 4)),
        "rs_out": dma((6, 3, 3)),
        "rs_in": dma((6, 3, 3)),
        "mom_out": dma((2,)),
        "mom_in": dma((2,)),
        "norm_out": dma((10,)),
        "norm_got": dma((10,)),
        "ag_out": dma((36,)),
        "ag_in": dma((36,)),
        "share_out": dma((30,)),
        "share_in": dma((30,)),
    }
    leaves, tree = jax.tree.flatten(scratch)

    def body(*refs):
        kernel(
            spans,
            rows,
            {"in": refs[:6], "out": refs[6:10], "scratch": jax.tree.unflatten(tree, refs[10:])},
        )

    whole = pl.BlockSpec(memory_space=pl.ANY)
    vmem = pl.BlockSpec(memory_space=pltpu.VMEM)
    return pl.pallas_call(
        body,
        name="adam_step",
        out_shape=(
            jax.ShapeDtypeStruct((rows, LANES), F32),
            jax.ShapeDtypeStruct((rows, LANES), F32),
            jax.ShapeDtypeStruct((rows, LANES), F32),
            jax.ShapeDtypeStruct((4, 4, 4, 2, rows, LANES), BF16),
        ),
        in_specs=[whole] * 5 + [pl.BlockSpec(memory_space=pltpu.SMEM)],
        out_specs=[vmem] * 4,
        scratch_shapes=leaves,
        compiler_params=pltpu.CompilerParams(collective_id=0, has_side_effects=True, vmem_limit_bytes=67_000_000),
    )(g, master, window, tail, head, bounds)


def local(grads, master, m_old, v_old, old_bounds):
    width = master.shape[0]
    rows, half = width // LANES, width // 2
    device = lax.axis_index(DP)
    begin = device * width - old_bounds[device]
    packed = jnp.concatenate([m_old, v_old])
    padded = jnp.pad(packed, ((0, 0), (width, 0)))

    def cut(offset, size):
        return lax.dynamic_slice_in_dim(padded, offset + width, size, 1).reshape(2, size // LANES, LANES)

    window = cut(begin, width)
    tail = cut(begin + width, half).astype(BF16)
    head = cut(begin - half, half).astype(BF16)
    master_new, m_new, v_new, params = step(
        grads.reshape(4, 4, 4, 2, rows, LANES), master.reshape(rows, LANES), window, tail, head, old_bounds
    )
    return master_new.reshape(width), m_new.reshape(width), v_new.reshape(width), params.reshape(128 * width)


def solution(mesh):
    finer = Mesh(mesh.devices.reshape(4, 4, 4, 2), DP)
    placed = (P(DP, None), P(DP), P(DP, None), P(DP, None), P())
    return jax.shard_map(local, mesh=finer, in_specs=placed, out_specs=(P(DP), P(DP), P(DP), P()), check_vma=False)
```

```python
import jax
import jax.numpy as jnp
from jax import lax
from jax.experimental import pallas as pl
from jax.experimental.pallas import tpu as pltpu
from jax.sharding import Mesh
from jax.sharding import PartitionSpec as P

DP = ("dz", "dy", "dx", "dc")
F32, BF16 = jnp.float32, jnp.bfloat16
LANES = 128
CUT = 64
ORDERS = ((2, 1, 0), (1, 0, 2), (0, 2, 1))
HALVES = ((48, 40), (48, 40), (40, 40))
SLOTS = (2, 1, 3, 0)
FAR, DIRECT, RELAY = 0, 1, 2


def plan(rows):
    spans, at = [], 0
    for pair in HALVES:
        colour = []
        for part in pair:
            size = part * rows // 256
            colour.append((at, size))
            at += size
        spans.append(colour)
    return spans


def kernel(spans, rows, refs):
    g, master, m_old, v_old, bounds = refs["in"]
    master_out, m_out, v_out, params = refs["out"]
    s = refs["scratch"]
    coords = [lax.axis_index(name) for name in DP[:3]]
    core = lax.axis_index("dc")
    other = 1 - core
    me = ((coords[0] * 4 + coords[1]) * 4 + coords[2]) * 2 + core

    def moved(dim, steps):
        at = list(coords)
        at[dim] = (coords[dim] + steps + 4) % 4
        return (*at, core)

    def located(index):
        return (index // 32, (index // 8) % 4, (index // 2) % 4, index % 2)

    partner = (*coords, other)
    after, before = located((me + 1) % 128), located((me + 127) % 128)
    beside = located((me + 127 + 2 * core) % 128)

    def remote(src, dst, send, recv, device):
        return pltpu.make_async_remote_copy(
            src_ref=src, dst_ref=dst, send_sem=send, recv_sem=recv, device_id=device, device_id_type=pl.DeviceIdType.MESH
        )

    def source(k, slot, parity):
        first = ORDERS[k][0]
        at = [slice(None)] * 3
        at[first] = (coords[first] + slot) % 4
        low = spans[k][0][0]
        size = spans[k][0][1] + spans[k][1][1]
        return g.at[at[0], at[1], at[2], parity, pl.ds(low, size)]

    loads = {}
    for slot in SLOTS:
        for k in range(3):
            loads[k, slot, 1] = pltpu.make_async_copy(source(k, slot, other), s["theirs"][k].at[slot], s["load"].at[k, slot, 1])
            loads[k, slot, 0] = pltpu.make_async_copy(source(k, slot, core), s["ours"][k].at[slot], s["load"].at[k, slot, 0])
            loads[k, slot, 1].start()
            loads[k, slot, 0].start()
    small = [
        pltpu.make_async_copy(master, s["master"], s["small"].at[0]),
        pltpu.make_async_copy(m_old, s["old"].at[0, pl.ds(rows, 2 * rows)], s["small"].at[1]),
        pltpu.make_async_copy(v_old, s["old"].at[1, pl.ds(rows, 2 * rows)], s["small"].at[1]),
    ]
    for copy in small:
        copy.start()

    barrier = pltpu.get_barrier_semaphore()
    peers = [moved(dim, step) for dim in range(3) for step in (1, 2, 3)] + [partner, beside]
    for peer in peers:
        pl.semaphore_signal(barrier, inc=1, device_id=peer, device_id_type=pl.DeviceIdType.MESH)
    pl.semaphore_wait(barrier, len(peers))

    def launch(copy):
        copy.start()
        return copy

    def settled(ref, sem):
        pltpu.make_async_copy(ref, ref, sem).wait()

    swaps = {}
    for slot in range(4):
        for k in range(3):
            swaps[k, slot] = remote(
                s["give"][k].at[slot], s["take"][k].at[slot], s["sent"].at[0], s["swap_in"].at[k, slot], partner
            )

    def narrow(k, slot):
        loads[k, slot, 1].wait()

        def body(t, carry):
            s["give"][k][slot, t // 4, t % 4] = s["theirs"][k][slot, t // 4, t % 4].astype(BF16)
            return carry

        lax.fori_loop(0, 16, body, 0)
        launch(swaps[k, slot])

    def joined(k, slot, h, t):
        u, v = (t // 4, t % 4) if ORDERS[k][1] < ORDERS[k][2] else (t % 4, t // 4)
        low = spans[k][h][0] - spans[k][0][0]
        at = pl.ds(low, spans[k][h][1])
        return s["ours"][k][slot, u, v, at] + s["take"][k][slot, u, v, at].astype(F32)

    def arrive(k, slot):
        loads[k, slot, 0].wait()
        swaps[k, slot].wait_recv()

    streams = [(k, h) for k in range(3) for h in range(2)]
    sign = {0: 1, 1: -1}

    def steps_of(h, phase):
        return ((FAR, 2 if phase == 2 else sign[h]), (DIRECT, -sign[h]), (RELAY, sign[h]))

    rs = {}
    for q, (k, h) in enumerate(streams):
        for phase in range(3):
            dim = ORDERS[k][phase]
            for kind, step in steps_of(h, phase):
                rs[q, phase, kind] = remote(
                    s["out"][q][phase].at[kind],
                    s["in"][q][phase].at[kind],
                    s["sent"].at[1 + phase],
                    s["rs_in"].at[q, phase, 0 if kind == FAR and phase < 2 else 1],
                    moved(dim, step),
                )

    def loop(count, body):
        def step(t, carry):
            body(t)
            return carry

        lax.fori_loop(0, count, step, 0)

    for k in range(3):
        narrow(k, 2)
    for k in range(3):
        narrow(k, 3)
        arrive(k, 2)
        for h in range(2):
            q = 2 * k + h

            def body(t, k=k, h=h, q=q):
                s["out"][q][0][FAR, t] = joined(k, 2, h, t).astype(BF16)

            loop(16, body)
            launch(rs[q, 0, FAR])
    for k in range(3):
        narrow(k, 1)
    for h, slot in ((0, 3), (1, 1)):
        for k in range(3):
            q = 2 * k + h
            arrive(k, slot)

            def body(t, k=k, h=h, q=q, slot=slot):
                s["out"][q][0][DIRECT, t] = joined(k, slot, h, t).astype(BF16)

            loop(16, body)
            launch(rs[q, 0, DIRECT])
    for k in range(3):
        narrow(k, 0)
    for q, (k, h) in enumerate(streams):
        rs[q, 0, FAR].wait_recv()

        def body(t, k=k, h=h, q=q):
            value = joined(k, sign[h] % 4, h, t) + s["in"][q][0][FAR, t].astype(F32)
            s["out"][q][0][RELAY, t] = value.astype(BF16)

        loop(16, body)
        launch(rs[q, 0, RELAY])

    moments_out = moments(s, rows, small, bounds, me, launch, remote, after, before)
    for k in range(3):
        arrive(k, 0)
    for q, (k, h) in enumerate(streams):
        settled(s["in"][q][0].at[pl.ds(DIRECT, 2)], s["rs_in"].at[q, 0, 1])

        def body(t, k=k, h=h, q=q):
            got = s["in"][q][0]
            s["sum"][q][0][t] = joined(k, 0, h, t) + got[DIRECT, t].astype(F32) + got[RELAY, t].astype(F32)

        loop(16, body)
        if True:
            second(s, rs, launch, loop, coords, q, k, h, sign, 1, 4)
    for q, (k, h) in enumerate(streams):
        relay(s, rs, launch, loop, coords, q, k, h, sign, 1, 4)
    for q, (k, h) in enumerate(streams):
        finish(s, rs, loop, coords, q, k, 1, 4)
        second(s, rs, launch, loop, coords, q, k, h, sign, 2, 1)
    total = jnp.zeros((8, LANES), F32)
    for q, (k, h) in enumerate(streams):
        finish(s, rs, loop, coords, q, k, 2, 1)
        value = s["sum"][q][2][0]
        square = value * value
        for i in range(spans[k][h][1] // 8):
            total += square[8 * i : 8 * i + 8]

    def merge():
        for copy in moments_out:
            copy.wait_recv()
        start = me * (rows * LANES)
        low, high = bounds[me] - start, bounds[me + 1] - start
        place = lax.broadcasted_iota(jnp.int32, (rows // 2, LANES), 0) * LANES + lax.broadcasted_iota(
            jnp.int32, (rows // 2, LANES), 1
        )
        for i in range(2):
            top, bottom = pl.ds(0, rows // 2), pl.ds(rows // 2, rows // 2)
            s["window"][i, top] = jnp.where(place < low, s["from_before"][i].astype(F32), s["window"][i, top])
            s["window"][i, bottom] = jnp.where(
                place + (rows // 2) * LANES >= high, s["from_after"][i].astype(F32), s["window"][i, bottom]
            )

    s["norm"][0] = jnp.sum(total, axis=0, keepdims=True)
    column = [(moved(0, step)[:3], c) for step in range(4) for c in (core, other)][1:]
    column = [(*place, c) for place, c in column]
    plane = [
        (coords[0], (coords[1] + y) % 4, (coords[2] + x) % 4, core) for y in range(4) for x in range(4)
    ][1:]
    for round_, group, base in ((0, column, 0), (1, plane, 7)):
        for i, device in enumerate(group):
            launch(
                remote(
                    s["norm"].at[round_],
                    s["norm_in"].at[base + i],
                    s["sent"].at[4],
                    s["norm_got"].at[round_],
                    device,
                )
            )
        value = s["norm"][round_]
        if round_ == 0:
            merge()
        settled(s["norm_in"].at[pl.ds(base, len(group))], s["norm_got"].at[round_])
        for i in range(len(group)):
            value += s["norm_in"][base + i]
        s["norm"][round_ + 1] = value
    norm = jnp.sum(s["norm"][2], axis=(0, 1), keepdims=True)
    clip = jnp.minimum(1.0, jnp.sqrt(F32(128 * rows * LANES)) / (jnp.sqrt(norm) + 1e-06))

    for q, (k, h) in enumerate(streams):
        at = pl.ds(*spans[k][h])
        clipped = clip * s["sum"][q][2][0]
        m_new = 0.5 * s["window"][0, at] + 0.5 * clipped
        v_new = 0.95 * s["window"][1, at] + 0.05 * clipped * clipped
        direction = m_new / (1.0 - 0.5**20) / (jnp.sqrt(v_new / (1.0 - 0.95**20)) + 1e-08)
        weights = s["master"][at]
        weights = weights - 0.05 * (direction + 0.1 * weights)
        master_out[at] = weights
        m_out[at] = m_new
        v_out[at] = v_new
        params[coords[0], coords[1], coords[2], core, at] = weights.astype(BF16)

    def spot(k, low, size, first, second_, third=None):
        at = [None] * 3
        one, two, three = ORDERS[k]
        at[one] = (coords[one] + first + 4) % 4
        at[two] = (coords[two] + second_ + 4) % 4
        at[three] = slice(None) if third is None else (coords[three] + third + 4) % 4
        return params.at[at[0], at[1], at[2], core, pl.ds(low, size)]

    def whole(k):
        return spans[k][0][0], spans[k][0][1] + spans[k][1][1]

    def share(k, first, second_):
        ref = spot(k, *whole(k), first, second_)
        launch(remote(ref, ref, s["sent"].at[8], s["shared"], partner))

    hops = {}

    def send(name, k, ref, dim, step):
        stage = {"third": 0, "second": 1, "second_far": 1, "first": 2, "first_far": 2}[name[0]]
        base = {"third": 0, "second": 1, "second_far": 3, "first": 4, "first_far": 12}[name[0]]
        rest = {"second": lambda i: i, "first": lambda line, i: 2 * line + i, "first_far": lambda line, i: line}
        i = base + rest.get(name[0], lambda i: 0)(*name[1:])
        hops[(k, *name)] = launch(remote(ref, ref, s["sent"].at[5 + stage], s["ag_in"].at[k, i], moved(dim, step)))

    around = ((0, 1), (1, -1))

    def forward(k, second_):
        for i, step in around:
            send(("first", second_ % 4, i), k, spot(k, *whole(k), 0, second_), ORDERS[k][0], step)

    def near(k, second_):
        for i, step in around:
            hops[k, "first", second_ % 4, i].wait_recv()
            send(("first_far", second_ % 4, i), k, spot(k, *spans[k][i], -step, second_), ORDERS[k][0], step)
            share(k, -step, second_)

    def far(k, second_):
        settled(spot(k, *whole(k), 2, second_), s["ag_in"].at[k, 12 + second_ % 4])
        share(k, 2, second_)

    for k in range(3):
        for i, step in enumerate((1, -1, 2)):
            send(("third", i), k, spot(k, *whole(k), 0, 0, 0), ORDERS[k][2], step)
    for k in range(3):
        settled(params.at[0, 0, pl.ds(0, 3), core, pl.ds(*whole(k))], s["ag_in"].at[k, 0])
        for i, step in around:
            send(("second", i), k, spot(k, *whole(k), 0, 0), ORDERS[k][1], step)
        forward(k, 0)
        share(k, 0, 0)
    for k in range(3):
        for i, step in around:
            hops[k, "second", i].wait_recv()
            send(("second_far", i), k, spot(k, *spans[k][i], 0, -step), ORDERS[k][1], step)
            forward(k, -step)
            share(k, 0, -step)
    for k in range(3):
        near(k, 0)
    for k in range(3):
        settled(spot(k, *whole(k), 0, 2), s["ag_in"].at[k, 3])
        forward(k, 2)
        share(k, 0, 2)
    for second_ in (1, -1, 2):
        for k in range(3):
            near(k, second_)
        for k in range(3):
            far(k, {1: 0, -1: 1, 2: -1}[second_])
    for k in range(3):
        far(k, 2)
    settled(params.at[:, :, :, other], s["shared"])
    lots = [params.at[pl.ds(0, 3), 0, 0, 0], params.at[pl.ds(0, 3), :, 0, 0], params.at[pl.ds(0, 3), :, :, 0]]
    everything = params.at[:, :, :, 0]
    for i, ref in enumerate([everything, *lots[::-1], s["norm_in"], *lots, everything]):
        settled(ref, s["sent"].at[i])
    for copy in moments_out:
        copy.wait_send()


def moments(s, rows, small, bounds, me, launch, remote, after, before):
    small[0].wait()
    loaded = s["old"].at[:, pl.ds(rows, 2 * rows)]
    pltpu.make_async_copy(loaded, loaded, s["small"].at[1]).wait()
    half = rows // 2
    begin = (me * rows + half) * LANES - bounds[me]
    begin = jnp.clip(begin, 0, rows * LANES)
    row, lane = begin // LANES, begin % LANES
    keep = lax.broadcasted_iota(jnp.int32, (CUT, LANES), 1) < LANES - lane
    blank = jnp.zeros((8, LANES), F32)
    for i in range(2):

        def clear(t, carry, i=i):
            s["old"][i, pl.ds(pl.multiple_of(8 * t, 8), 8)] = blank
            return carry

        lax.fori_loop(0, rows // 8, clear, 0)
        s["old"][i, 3 * rows : 3 * rows + 8] = blank

        def shifted(at, i=i):
            first = s["old"][i, pl.ds(row + at, CUT)]
            second = s["old"][i, pl.ds(row + at + 1, CUT)]
            return jnp.where(keep, pltpu.roll(first, LANES - lane, 1), pltpu.roll(second, LANES - lane, 1))

        def ends(t, carry, i=i, shifted=shifted):
            at = pl.multiple_of(CUT * t, CUT)
            for ref, base in ((s["head"], 0), (s["tail"], half + rows)):
                ref[i, pl.ds(at, CUT)] = shifted(base + at).astype(BF16)
            return carry

        lax.fori_loop(0, half // CUT, ends, 0)

        def middle(t, carry, i=i, shifted=shifted):
            at = pl.multiple_of(CUT * t, CUT)
            s["window"][i, pl.ds(at, CUT)] = shifted(half + at)
            return carry

        lax.fori_loop(0, rows // CUT, middle, 0)
    return [
        launch(remote(s["tail"], s["from_before"], s["mom_out"].at[0], s["mom_in"].at[0], after)),
        launch(remote(s["head"], s["from_after"], s["mom_out"].at[1], s["mom_in"].at[1], before)),
    ]


def second(s, rs, launch, loop, coords, q, k, h, sign, phase, count):
    place = coords[ORDERS[k][phase]]
    pieces = ((FAR, 2), (DIRECT, -sign[h]), (RELAY, sign[h]))
    for kind, step in pieces[: phase + 1]:
        at = ((place + step + 4) % 4) * count

        def body(t, kind=kind, at=at):
            s["out"][q][phase][kind, t] = s["sum"][q][phase - 1][at + t].astype(BF16)

        loop(count, body)
        launch(rs[q, phase, kind])


def relay(s, rs, launch, loop, coords, q, k, h, sign, phase, count):
    place = coords[ORDERS[k][phase]]
    rs[q, phase, FAR].wait_recv()
    at = ((place + sign[h] + 4) % 4) * count

    def body(t):
        value = s["sum"][q][phase - 1][at + t] + s["in"][q][phase][FAR, t].astype(F32)
        s["out"][q][phase][RELAY, t] = value.astype(BF16)

    loop(count, body)
    launch(rs[q, phase, RELAY])


def finish(s, rs, loop, coords, q, k, phase, count):
    place = coords[ORDERS[k][phase]]
    kinds = (FAR, DIRECT, RELAY) if phase == 2 else (DIRECT, RELAY)
    arrived = s["in"][q][phase].at[pl.ds(kinds[0], len(kinds))]
    pltpu.make_async_copy(arrived, arrived, s["rs_in"].at[q, phase, 1]).wait()
    at = place * count

    def body(t):
        value = s["sum"][q][phase - 1][at + t]
        for kind in kinds:
            value += s["in"][q][phase][kind, t].astype(F32)
        s["sum"][q][phase][t] = value

    loop(count, body)


def step(g, master, m_old, v_old, bounds):
    rows = master.shape[0]
    spans = plan(rows)
    sizes = [a[1] + b[1] for a, b in spans]
    dma = pltpu.SemaphoreType.DMA
    halves = [span for colour in spans for span in colour]
    scratch = {
        "theirs": [pltpu.VMEM((4, 4, 4, n, LANES), F32) for n in sizes],
        "ours": [pltpu.VMEM((4, 4, 4, n, LANES), F32) for n in sizes],
        "give": [pltpu.VMEM((4, 4, 4, n, LANES), BF16) for n in sizes],
        "take": [pltpu.VMEM((4, 4, 4, n, LANES), BF16) for n in sizes],
        "out": [[pltpu.VMEM((3, m, n, LANES), BF16) for m in (16, 4, 1)] for _, n in halves],
        "in": [[pltpu.VMEM((3, m, n, LANES), BF16) for m in (16, 4, 1)] for _, n in halves],
        "sum": [[pltpu.VMEM((m, n, LANES), F32) for m in (16, 4, 1)] for _, n in halves],
        "master": pltpu.VMEM((rows, LANES), F32),
        "old": pltpu.VMEM((2, 3 * rows + 8, LANES), F32),
        "window": pltpu.VMEM((2, rows, LANES), F32),
        "tail": pltpu.VMEM((2, rows // 2, LANES), BF16),
        "head": pltpu.VMEM((2, rows // 2, LANES), BF16),
        "from_before": pltpu.VMEM((2, rows // 2, LANES), BF16),
        "from_after": pltpu.VMEM((2, rows // 2, LANES), BF16),
        "norm": pltpu.VMEM((3, 1, LANES), F32),
        "norm_in": pltpu.VMEM((22, 1, LANES), F32),
        "load": dma((3, 4, 2)),
        "small": dma((2,)),
        "swap_in": dma((3, 4)),
        "sent": dma((9,)),
        "rs_in": dma((6, 3, 2)),
        "mom_out": dma((2,)),
        "mom_in": dma((2,)),
        "norm_got": dma((2,)),
        "ag_in": dma((3, 16)),
        "shared": dma(()),
    }
    leaves, tree = jax.tree.flatten(scratch)

    def body(*refs):
        kernel(
            spans,
            rows,
            {"in": refs[:5], "out": refs[5:9], "scratch": jax.tree.unflatten(tree, refs[9:])},
        )

    whole = pl.BlockSpec(memory_space=pl.ANY)
    vmem = pl.BlockSpec(memory_space=pltpu.VMEM)
    return pl.pallas_call(
        body,
        name="adam_step",
        out_shape=(
            pltpu.VMEM((rows, LANES), F32),
            pltpu.VMEM((rows, LANES), F32),
            pltpu.VMEM((rows, LANES), F32),
            pltpu.VMEM((4, 4, 4, 2, rows, LANES), BF16),
        ),
        in_specs=[whole] * 4 + [pl.BlockSpec(memory_space=pltpu.SMEM)],
        out_specs=[vmem] * 4,
        scratch_shapes=leaves,
        compiler_params=pltpu.CompilerParams(collective_id=0, has_side_effects=True, vmem_limit_bytes=48 * 2**20),
    )(g, master, m_old, v_old, bounds)


def flush_body(*refs):
    count = len(refs) // 2
    copies = [pltpu.make_async_copy(refs[i], refs[count + i], refs[-1].at[i]) for i in range(count)]
    for copy in copies:
        copy.start()
    for copy in copies:
        copy.wait()


def flush(arrays):
    return pl.pallas_call(
        flush_body,
        name="flush",
        out_shape=tuple(jax.ShapeDtypeStruct(a.shape, a.dtype) for a in arrays),
        in_specs=[pl.BlockSpec(memory_space=pltpu.VMEM)] * len(arrays),
        out_specs=[pl.BlockSpec(memory_space=pl.ANY)] * len(arrays),
        scratch_shapes=[pltpu.SemaphoreType.DMA((len(arrays),))],
        compiler_params=pltpu.CompilerParams(vmem_limit_bytes=2**20),
    )(*arrays)


def local(grads, master, m_old, v_old, old_bounds):
    width = master.shape[0]
    rows = width // LANES
    results = step(
        grads.reshape(4, 4, 4, 2, rows, LANES),
        master.reshape(rows, LANES),
        m_old.reshape(2 * rows, LANES),
        v_old.reshape(2 * rows, LANES),
        old_bounds,
    )
    return tuple(a.reshape(-1) for a in flush(results))


def solution(mesh):
    finer = Mesh(mesh.devices.reshape(4, 4, 4, 2), DP)
    placed = (P(DP, None), P(DP), P(DP, None), P(DP, None), P())
    return jax.shard_map(local, mesh=finer, in_specs=placed, out_specs=(P(DP), P(DP), P(DP), P()), check_vma=False)
```

```python
import jax
import jax.numpy as jnp
from jax import lax
from jax.experimental import pallas as pl
from jax.experimental.pallas import tpu as pltpu
from jax.sharding import Mesh
from jax.sharding import PartitionSpec as P

DP = ("dz", "dy", "dx", "dc")
F32, BF16 = jnp.float32, jnp.bfloat16
LANES = 128
CUT = 64
ORDERS = ((2, 1, 0), (1, 0, 2), (0, 2, 1))
HALVES = ((48, 40), (48, 40), (40, 40))
SLOTS = (2, 1, 3, 0)
FAR, DIRECT, RELAY = 0, 1, 2


def plan(rows):
    spans, at = [], 0
    for pair in HALVES:
        colour = []
        for part in pair:
            size = part * rows // 256
            colour.append((at, size))
            at += size
        spans.append(colour)
    return spans


def kernel(spans, rows, refs):
    g, master, m_old, v_old, bounds = refs["in"]
    master_out, m_out, v_out, params = refs["out"]
    s = refs["scratch"]
    coords = [lax.axis_index(name) for name in DP[:3]]
    core = lax.axis_index("dc")
    other = 1 - core
    me = ((coords[0] * 4 + coords[1]) * 4 + coords[2]) * 2 + core

    def moved(dim, steps):
        at = list(coords)
        at[dim] = (coords[dim] + steps + 4) % 4
        return (*at, core)

    def located(index):
        return (index // 32, (index // 8) % 4, (index // 2) % 4, index % 2)

    partner = (*coords, other)
    after, before = located((me + 1) % 128), located((me + 127) % 128)
    beside = located((me + 127 + 2 * core) % 128)

    def remote(src, dst, send, recv, device):
        return pltpu.make_async_remote_copy(
            src_ref=src, dst_ref=dst, send_sem=send, recv_sem=recv, device_id=device, device_id_type=pl.DeviceIdType.MESH
        )

    def source(k, slot, parity):
        first = ORDERS[k][0]
        at = [slice(None)] * 3
        at[first] = (coords[first] + slot) % 4
        low = spans[k][0][0]
        size = spans[k][0][1] + spans[k][1][1]
        return g.at[at[0], at[1], at[2], parity, pl.ds(low, size)]

    loads = {}
    for slot in SLOTS:
        for k in range(3):
            loads[k, slot, 1] = pltpu.make_async_copy(source(k, slot, other), s["theirs"][k].at[slot], s["load"].at[k, slot, 1])
            loads[k, slot, 0] = pltpu.make_async_copy(source(k, slot, core), s["ours"][k].at[slot], s["load"].at[k, slot, 0])
            loads[k, slot, 1].start()
            loads[k, slot, 0].start()
    small = [
        pltpu.make_async_copy(master, s["master"], s["small"].at[0]),
        pltpu.make_async_copy(m_old, s["old"].at[0, pl.ds(rows, 2 * rows)], s["small"].at[1]),
        pltpu.make_async_copy(v_old, s["old"].at[1, pl.ds(rows, 2 * rows)], s["small"].at[1]),
    ]
    for copy in small:
        copy.start()

    barrier = pltpu.get_barrier_semaphore()
    peers = [moved(dim, step) for dim in range(3) for step in (1, 2, 3)] + [partner, beside]
    for peer in peers:
        pl.semaphore_signal(barrier, inc=1, device_id=peer, device_id_type=pl.DeviceIdType.MESH)
    pl.semaphore_wait(barrier, len(peers))

    def launch(copy):
        copy.start()
        return copy

    def settled(ref, sem):
        pltpu.make_async_copy(ref, ref, sem).wait()

    swaps = {}
    for slot in range(4):
        for k in range(3):
            swaps[k, slot] = remote(
                s["give"][k].at[slot], s["take"][k].at[slot], s["sent"].at[0], s["swap_in"].at[k, slot], partner
            )

    def narrow(k, slot):
        loads[k, slot, 1].wait()

        def body(t, carry):
            s["give"][k][slot, t // 4, t % 4] = s["theirs"][k][slot, t // 4, t % 4].astype(BF16)
            return carry

        lax.fori_loop(0, 16, body, 0)
        launch(swaps[k, slot])

    def joined(k, slot, h, second, third):
        _, two, three = ORDERS[k]
        i2, i3 = (coords[two] + second) % 4, (coords[three] + third) % 4
        u, v = (i2, i3) if two < three else (i3, i2)
        at = pl.ds(spans[k][h][0] - spans[k][0][0], spans[k][h][1])
        return s["ours"][k][slot, u, v, at] + s["take"][k][slot, u, v, at].astype(F32)

    def arrive(k, slot):
        loads[k, slot, 0].wait()
        swaps[k, slot].wait_recv()

    streams = [(k, h) for k in range(3) for h in range(2)]
    sign = {0: 1, 1: -1}

    def hop(q, phase, kind, line=None):
        k, h = streams[q]
        step = {FAR: 2 if phase == 2 else sign[h], DIRECT: -sign[h], RELAY: sign[h]}[kind]
        src, dst = s["out"][q][phase].at[kind], s["in"][q][phase].at[kind]
        group = 0 if kind == FAR and phase < 2 else 1
        got = s["rs_in"].at[q, max(phase - 1, 0), group]
        if line is not None:
            src, dst = src.at[pl.ds(4 * line, 4)], dst.at[pl.ds(4 * line, 4)]
            got = s["rs_line"].at[q, group, line]
        return remote(src, dst, s["sent"].at[1 + phase], got, moved(ORDERS[k][phase], step))

    def loop(count, body):
        def step(t, carry):
            body(t)
            return carry

        lax.fori_loop(0, count, step, 0)

    def first(q, kind, place):
        k, h = streams[q]
        line = order[h][place]
        slot = {FAR: 2, DIRECT: -sign[h] % 4, RELAY: sign[h] % 4}[kind]
        if kind == RELAY:
            hop(q, 0, FAR, line).wait_recv()

        def body(t):
            value = joined(k, slot, h, line, t)
            if kind == RELAY:
                value += s["in"][q][0][FAR, 4 * line + t].astype(F32)
            s["out"][q][0][kind, 4 * line + t] = value.astype(BF16)

        loop(4, body)
        launch(hop(q, 0, kind, line))

    def finished(q, place):
        k, h = streams[q]
        line = order[h][place]
        settled(s["in"][q][0].at[pl.ds(DIRECT, 2), pl.ds(4 * line, 4)], s["rs_line"].at[q, 1, line])

        def body(t):
            got = s["in"][q][0]
            value = joined(k, 0, h, line, t)
            value += got[DIRECT, 4 * line + t].astype(F32) + got[RELAY, 4 * line + t].astype(F32)
            if place < 2:
                s["out"][q][1][(FAR, DIRECT)[place], t] = value.astype(BF16)
            else:
                s["sum"][q][0][place - 2, t] = value

        loop(4, body)
        if place < 2:
            launch(hop(q, 1, (FAR, DIRECT)[place]))

    def relayed(q):
        hop(q, 1, FAR).wait_recv()

        def body(t):
            value = s["sum"][q][0][0, t] + s["in"][q][1][FAR, t].astype(F32)
            s["out"][q][1][RELAY, t] = value.astype(BF16)

        loop(4, body)
        launch(hop(q, 1, RELAY))

    def second(q):
        _, h = streams[q]
        settled(s["in"][q][1].at[pl.ds(DIRECT, 2)], s["rs_in"].at[q, 0, 1])
        for kind, third in ((FAR, 2), (DIRECT, -sign[h] % 4), (RELAY, sign[h] % 4), (None, 0)):
            got = s["in"][q][1]
            value = s["sum"][q][0][1, third] + got[DIRECT, third].astype(F32) + got[RELAY, third].astype(F32)
            if kind is None:
                s["sum"][q][1][...] = value
            else:
                s["out"][q][2][kind, 0] = value.astype(BF16)
                launch(hop(q, 2, kind))

    def third(q):
        got = s["in"][q][2]
        settled(got, s["rs_in"].at[q, 1, 1])
        value = s["sum"][q][1][...]
        for kind in (FAR, DIRECT, RELAY):
            value += got[kind, 0].astype(F32)
        s["sum"][q][2][...] = value
        return value * value

    order = [(2, -sign[h] % 4, sign[h] % 4, 0) for h in range(2)]
    for k in range(3):
        narrow(k, 2)
    for k in range(3):
        narrow(k, 3)
        arrive(k, 2)
        for h in range(2):
            for place in range(4):
                first(2 * k + h, FAR, place)
    for k in range(3):
        narrow(k, 1)
    for h in range(2):
        for k in range(3):
            arrive(k, -sign[h] % 4)
            for place in range(2):
                first(2 * k + h, DIRECT, place)
    for k in range(3):
        narrow(k, 0)
    for kind, place in ((RELAY, 0), (DIRECT, 2), (RELAY, 1), (DIRECT, 3)):
        for q in range(6):
            first(q, kind, place)
    moments_out = moments(s, rows, small, bounds, me, launch, remote, after, before)
    for q in range(6):
        first(q, RELAY, 2)
    for k in range(3):
        arrive(k, 0)
    for q in range(6):
        finished(q, 0)
    for q in range(6):
        first(q, RELAY, 3)
    for q in range(6):
        finished(q, 1)
    for q in range(6):
        finished(q, 2)
        relayed(q)
    for q in range(6):
        finished(q, 3)
    for q in range(6):
        second(q)
    total = jnp.zeros((8, LANES), F32)
    for q, (k, h) in enumerate(streams):
        square = third(q)
        for i in range(spans[k][h][1] // 8):
            total += square[8 * i : 8 * i + 8]

    def merge():
        for copy in moments_out:
            copy.wait_recv()
        start = me * (rows * LANES)
        low, high = bounds[me] - start, bounds[me + 1] - start
        place = lax.broadcasted_iota(jnp.int32, (rows // 2, LANES), 0) * LANES + lax.broadcasted_iota(
            jnp.int32, (rows // 2, LANES), 1
        )
        for i in range(2):
            top, bottom = pl.ds(0, rows // 2), pl.ds(rows // 2, rows // 2)
            s["window"][i, top] = jnp.where(place < low, s["from_before"][i].astype(F32), s["window"][i, top])
            s["window"][i, bottom] = jnp.where(
                place + (rows // 2) * LANES >= high, s["from_after"][i].astype(F32), s["window"][i, bottom]
            )

    s["norm"][0] = jnp.sum(total, axis=0, keepdims=True)
    column = [(moved(0, step)[:3], c) for step in range(4) for c in (core, other)][1:]
    column = [(*place, c) for place, c in column]
    plane = [
        (coords[0], (coords[1] + y) % 4, (coords[2] + x) % 4, core) for y in range(4) for x in range(4)
    ][1:]
    for round_, group, base in ((0, column, 0), (1, plane, 7)):
        for i, device in enumerate(group):
            launch(
                remote(
                    s["norm"].at[round_],
                    s["norm_in"].at[base + i],
                    s["sent"].at[4],
                    s["norm_got"].at[round_],
                    device,
                )
            )
        value = s["norm"][round_]
        if round_ == 0:
            merge()
        settled(s["norm_in"].at[pl.ds(base, len(group))], s["norm_got"].at[round_])
        for i in range(len(group)):
            value += s["norm_in"][base + i]
        s["norm"][round_ + 1] = value
    norm = jnp.sum(s["norm"][2], axis=(0, 1), keepdims=True)
    clip = jnp.minimum(1.0, jnp.sqrt(F32(128 * rows * LANES)) / (jnp.sqrt(norm) + 1e-06))

    for q, (k, h) in enumerate(streams):
        at = pl.ds(*spans[k][h])
        clipped = clip * s["sum"][q][2][...]
        m_new = 0.5 * s["window"][0, at] + 0.5 * clipped
        v_new = 0.95 * s["window"][1, at] + 0.05 * clipped * clipped
        direction = m_new / (1.0 - 0.5**20) / (jnp.sqrt(v_new / (1.0 - 0.95**20)) + 1e-08)
        weights = s["master"][at]
        weights = weights - 0.05 * (direction + 0.1 * weights)
        master_out[at] = weights
        m_out[at] = m_new
        v_out[at] = v_new
        params[coords[0], coords[1], coords[2], core, at] = weights.astype(BF16)

    def spot(k, low, size, first, second_, third=None):
        at = [None] * 3
        one, two, three = ORDERS[k]
        at[one] = (coords[one] + first + 4) % 4
        at[two] = (coords[two] + second_ + 4) % 4
        at[three] = slice(None) if third is None else (coords[three] + third + 4) % 4
        return params.at[at[0], at[1], at[2], core, pl.ds(low, size)]

    def whole(k):
        return spans[k][0][0], spans[k][0][1] + spans[k][1][1]

    def share(k, first, second_):
        ref = spot(k, *whole(k), first, second_)
        launch(remote(ref, ref, s["sent"].at[8], s["shared"], partner))

    hops = {}

    def send(name, k, ref, dim, step):
        stage = {"third": 0, "second": 1, "second_far": 1, "first": 2, "first_far": 2}[name[0]]
        base = {"third": 0, "second": 1, "second_far": 3, "first": 4, "first_far": 12}[name[0]]
        rest = {"second": lambda i: i, "first": lambda line, i: 2 * line + i, "first_far": lambda line, i: line}
        i = base + rest.get(name[0], lambda i: 0)(*name[1:])
        hops[(k, *name)] = launch(remote(ref, ref, s["sent"].at[5 + stage], s["ag_in"].at[k, i], moved(dim, step)))

    around = ((0, 1), (1, -1))

    def forward(k, second_):
        for i, step in around:
            send(("first", second_ % 4, i), k, spot(k, *whole(k), 0, second_), ORDERS[k][0], step)

    def near(k, second_):
        for i, step in around:
            hops[k, "first", second_ % 4, i].wait_recv()
            send(("first_far", second_ % 4, i), k, spot(k, *spans[k][i], -step, second_), ORDERS[k][0], step)
            share(k, -step, second_)

    def far(k, second_):
        settled(spot(k, *whole(k), 2, second_), s["ag_in"].at[k, 12 + second_ % 4])
        share(k, 2, second_)

    for k in range(3):
        for i, step in enumerate((1, -1, 2)):
            send(("third", i), k, spot(k, *whole(k), 0, 0, 0), ORDERS[k][2], step)
    for k in range(3):
        settled(params.at[0, 0, pl.ds(0, 3), core, pl.ds(*whole(k))], s["ag_in"].at[k, 0])
        for i, step in around:
            send(("second", i), k, spot(k, *whole(k), 0, 0), ORDERS[k][1], step)
    for k in range(3):
        forward(k, 0)
        share(k, 0, 0)
    for k in range(3):
        for i, step in around:
            hops[k, "second", i].wait_recv()
            send(("second_far", i), k, spot(k, *spans[k][i], 0, -step), ORDERS[k][1], step)
    for k in range(3):
        for i, step in around:
            forward(k, -step)
            share(k, 0, -step)
    for k in range(3):
        near(k, 0)
    for k in range(3):
        settled(spot(k, *whole(k), 0, 2), s["ag_in"].at[k, 3])
        forward(k, 2)
        share(k, 0, 2)
    for second_ in (1, -1, 2):
        for k in range(3):
            near(k, second_)
        for k in range(3):
            far(k, {1: 0, -1: 1, 2: -1}[second_])
    for k in range(3):
        far(k, 2)
    settled(params.at[:, :, :, other], s["shared"])
    lots = [params.at[pl.ds(0, 3), 0, 0, 0], params.at[pl.ds(0, 3), :, 0, 0], params.at[pl.ds(0, 3), :, :, 0]]
    everything = params.at[:, :, :, 0]
    for i, ref in enumerate([everything, *lots[::-1], s["norm_in"], *lots, everything]):
        settled(ref, s["sent"].at[i])
    for copy in moments_out:
        copy.wait_send()


def moments(s, rows, small, bounds, me, launch, remote, after, before):
    small[0].wait()
    loaded = s["old"].at[:, pl.ds(rows, 2 * rows)]
    pltpu.make_async_copy(loaded, loaded, s["small"].at[1]).wait()
    half = rows // 2
    begin = (me * rows + half) * LANES - bounds[me]
    begin = jnp.clip(begin, 0, rows * LANES)
    row, lane = begin // LANES, begin % LANES
    keep = lax.broadcasted_iota(jnp.int32, (CUT, LANES), 1) < LANES - lane
    blank = jnp.zeros((8, LANES), F32)
    for i in range(2):

        def clear(t, carry, i=i):
            s["old"][i, pl.ds(pl.multiple_of(8 * t, 8), 8)] = blank
            return carry

        lax.fori_loop(0, rows // 8, clear, 0)
        s["old"][i, 3 * rows : 3 * rows + 8] = blank

        def shifted(at, i=i):
            first = s["old"][i, pl.ds(row + at, CUT)]
            second = s["old"][i, pl.ds(row + at + 1, CUT)]
            return jnp.where(keep, pltpu.roll(first, LANES - lane, 1), pltpu.roll(second, LANES - lane, 1))

        def ends(t, carry, i=i, shifted=shifted):
            at = pl.multiple_of(CUT * t, CUT)
            for ref, base in ((s["head"], 0), (s["tail"], half + rows)):
                ref[i, pl.ds(at, CUT)] = shifted(base + at).astype(BF16)
            return carry

        lax.fori_loop(0, half // CUT, ends, 0)

        def middle(t, carry, i=i, shifted=shifted):
            at = pl.multiple_of(CUT * t, CUT)
            s["window"][i, pl.ds(at, CUT)] = shifted(half + at)
            return carry

        lax.fori_loop(0, rows // CUT, middle, 0)
    return [
        launch(remote(s["tail"], s["from_before"], s["mom_out"].at[0], s["mom_in"].at[0], after)),
        launch(remote(s["head"], s["from_after"], s["mom_out"].at[1], s["mom_in"].at[1], before)),
    ]


def step(g, master, m_old, v_old, bounds):
    rows = master.shape[0]
    spans = plan(rows)
    sizes = [a[1] + b[1] for a, b in spans]
    dma = pltpu.SemaphoreType.DMA
    halves = [span for colour in spans for span in colour]
    scratch = {
        "theirs": [pltpu.VMEM((4, 4, 4, n, LANES), F32) for n in sizes],
        "ours": [pltpu.VMEM((4, 4, 4, n, LANES), F32) for n in sizes],
        "give": [pltpu.VMEM((4, 4, 4, n, LANES), BF16) for n in sizes],
        "take": [pltpu.VMEM((4, 4, 4, n, LANES), BF16) for n in sizes],
        "out": [[pltpu.VMEM((3, m, n, LANES), BF16) for m in (16, 4, 1)] for _, n in halves],
        "in": [[pltpu.VMEM((3, m, n, LANES), BF16) for m in (16, 4, 1)] for _, n in halves],
        "sum": [
            [pltpu.VMEM((2, 4, n, LANES), F32), pltpu.VMEM((n, LANES), F32), pltpu.VMEM((n, LANES), F32)] for _, n in halves
        ],
        "master": pltpu.VMEM((rows, LANES), F32),
        "old": pltpu.VMEM((2, 3 * rows + 8, LANES), F32),
        "window": pltpu.VMEM((2, rows, LANES), F32),
        "tail": pltpu.VMEM((2, rows // 2, LANES), BF16),
        "head": pltpu.VMEM((2, rows // 2, LANES), BF16),
        "from_before": pltpu.VMEM((2, rows // 2, LANES), BF16),
        "from_after": pltpu.VMEM((2, rows // 2, LANES), BF16),
        "norm": pltpu.VMEM((3, 1, LANES), F32),
        "norm_in": pltpu.VMEM((22, 1, LANES), F32),
        "load": dma((3, 4, 2)),
        "small": dma((2,)),
        "swap_in": dma((3, 4)),
        "sent": dma((9,)),
        "rs_line": dma((6, 2, 4)),
        "rs_in": dma((6, 2, 2)),
        "mom_out": dma((2,)),
        "mom_in": dma((2,)),
        "norm_got": dma((2,)),
        "ag_in": dma((3, 16)),
        "shared": dma(()),
    }
    leaves, tree = jax.tree.flatten(scratch)

    def body(*refs):
        kernel(
            spans,
            rows,
            {"in": refs[:5], "out": refs[5:9], "scratch": jax.tree.unflatten(tree, refs[9:])},
        )

    whole = pl.BlockSpec(memory_space=pl.ANY)
    vmem = pl.BlockSpec(memory_space=pltpu.VMEM)
    return pl.pallas_call(
        body,
        name="adam_step",
        out_shape=(
            pltpu.VMEM((rows, LANES), F32),
            pltpu.VMEM((rows, LANES), F32),
            pltpu.VMEM((rows, LANES), F32),
            pltpu.VMEM((4, 4, 4, 2, rows, LANES), BF16),
        ),
        in_specs=[whole] * 4 + [pl.BlockSpec(memory_space=pltpu.SMEM)],
        out_specs=[vmem] * 4,
        scratch_shapes=leaves,
        compiler_params=pltpu.CompilerParams(collective_id=0, has_side_effects=True, vmem_limit_bytes=48 * 2**20),
    )(g, master, m_old, v_old, bounds)


def flush_body(*refs):
    count = len(refs) // 2
    copies = [pltpu.make_async_copy(refs[i], refs[count + i], refs[-1].at[i]) for i in range(count)]
    for copy in copies:
        copy.start()
    for copy in copies:
        copy.wait()


def flush(arrays):
    return pl.pallas_call(
        flush_body,
        name="flush",
        out_shape=tuple(jax.ShapeDtypeStruct(a.shape, a.dtype) for a in arrays),
        in_specs=[pl.BlockSpec(memory_space=pltpu.VMEM)] * len(arrays),
        out_specs=[pl.BlockSpec(memory_space=pl.ANY)] * len(arrays),
        scratch_shapes=[pltpu.SemaphoreType.DMA((len(arrays),))],
        compiler_params=pltpu.CompilerParams(vmem_limit_bytes=2**20),
    )(*arrays)


def local(grads, master, m_old, v_old, old_bounds):
    width = master.shape[0]
    rows = width // LANES
    results = step(
        grads.reshape(4, 4, 4, 2, rows, LANES),
        master.reshape(rows, LANES),
        m_old.reshape(2 * rows, LANES),
        v_old.reshape(2 * rows, LANES),
        old_bounds,
    )
    return tuple(a.reshape(-1) for a in flush(results))


def solution(mesh):
    finer = Mesh(mesh.devices.reshape(4, 4, 4, 2), DP)
    placed = (P(DP, None), P(DP), P(DP, None), P(DP, None), P())
    return jax.shard_map(local, mesh=finer, in_specs=placed, out_specs=(P(DP), P(DP), P(DP), P()), check_vma=False)
```
